32 devices in a mesh: dp: 4 (over x, core), expert: 8 (over z, y).
Axes of the slice: x: 2, y: 2, z: 4, core: 2. Of those that a mesh axis runs over, the one named last changes fastest.
Arguments:
- tokens: bfloat16 [128, 256, 1280], P(('dp', 'expert')), may hold values from -32 to 32
- slot_keys: bfloat16 [1280, 8], replicated, may hold values from -20 to 20
- logit_scale: float32 [1], replicated, may hold values from 8 to 16
- up_weight: bfloat16 [8, 1280, 5120], P('expert', None, 'dp'), may hold values from -0.15625 to 0.15625
- up_bias: bfloat16 [8, 5120], P('expert', 'dp'), may hold values from -3 to 3
- down_weight: bfloat16 [8, 5120, 1280], P('expert', 'dp'), may hold values from -0.078125 to 0.078125
- down_bias: bfloat16 [8, 1280], replicated, may hold values from -3 to 3
Outputs:
- mixed_out: bfloat16 [128, 256, 1280], P(('dp', 'expert'))
The draws below stay inside these ranges and needn't reach their ends.
All inputs are finite; a program needn't handle non-finite values.
Results may differ from the reference program's by a relative error of at most 0.017.
Values may be sent and summed in bfloat16 or wider, within the bound.
A program may use at most 64 MiB of HBM per device.

```python
import math
import jax
import jax.numpy as jnp
from jax import lax

D = 1280
FF = 5120
PATCHES = 256
EXPERTS = 8
IMAGES = 128
N_DP = 4


def slot_basis(key):
    raw = jax.random.normal(jax.random.fold_in(key, 11), (D, EXPERTS), jnp.float32)
    return jnp.clip(raw, -4.0, 4.0)


def draw_slot_keys(key, part):
    basis = slot_basis(key)
    column_scale = jnp.exp(jax.random.uniform(jax.random.fold_in(key, 12), (1, EXPERTS), jnp.float32, math.log(0.5), math.log(5.0)))
    return (basis * column_scale).astype(jnp.bfloat16)


def draw_tokens(key, part):
    basis = slot_basis(key)
    rows_total = IMAGES * PATCHES
    coeffs = jnp.clip(jax.random.normal(jax.random.fold_in(key, 13), (rows_total, EXPERTS), jnp.float32), -4.0, 4.0)
    mixture = 0.2 * jnp.dot(coeffs, jnp.transpose(basis))
    noise = jnp.clip(jax.random.normal(jax.random.fold_in(key, 14), (rows_total, D), jnp.float32), -4.0, 4.0)
    row_scale = jnp.exp(jax.random.uniform(jax.random.fold_in(key, 15), (rows_total, 1), jnp.float32, math.log(0.5), math.log(5.0)))
    values = jnp.clip(row_scale * (noise + mixture), -32.0, 32.0)
    return values.reshape(IMAGES, PATCHES, D).astype(jnp.bfloat16)


def level_of(own_key, shape, pieces, smallest, largest):
    factor_of = 1.0
    for dim, blocks in pieces:
        draws = jax.random.uniform(jax.random.fold_in(jax.random.fold_in(own_key, 6), dim), (blocks,), jnp.float32, smallest / len(pieces), largest / len(pieces))
        factor_of = factor_of * jnp.repeat(jnp.exp(draws), shape[dim] // blocks).reshape((-1,) + (1,) * (len(shape) - 1 - dim))
    return factor_of


def bell_draw(key, dims, scale, bound, cuts=(), held_as=jnp.bfloat16):
    entries = scale * jax.random.normal(key, dims, jnp.float32)
    if cuts:
        entries = entries * level_of(key, dims, cuts, -0.22, 0.18)
    return jnp.clip(entries, -bound, bound).astype(held_as)


def setup_inputs(seed: int = 0) -> dict:
    key_list = jax.random.split(jax.random.key(seed), 8)
    tokens = draw_tokens(jax.random.fold_in(key_list[7], 71), 0)
    slot_keys = draw_slot_keys(jax.random.fold_in(key_list[7], 71), 0)
    logit_scale = jnp.clip(jnp.exp(jax.random.uniform(key_list[2], (1,), jnp.float32, math.log(8.0), math.log(16.0))), 8.0, 16.0)
    up_weight = bell_draw(key_list[3], (EXPERTS, D, FF), D ** -0.5, 0.15625, ((0, 8), (2, 4)))
    up_bias = bell_draw(key_list[4], (EXPERTS, FF), 0.5, 3.0, ((0, 8), (1, 4)))
    down_weight = bell_draw(key_list[5], (EXPERTS, FF, D), FF ** -0.5, 0.078125, ((0, 8), (1, 4)))
    down_bias = bell_draw(key_list[6], (EXPERTS, D), 0.5, 3.0)
    return dict(tokens=tokens, slot_keys=slot_keys, logit_scale=logit_scale, up_weight=up_weight, up_bias=up_bias, down_weight=down_weight, down_bias=down_bias)


norm_eps = 1e-06

def unit_rms(values, axis_pos):
    return values * lax.rsqrt(lax.optimization_barrier(jnp.mean(values * values, axis=axis_pos, keepdims=True)) + norm_eps)

def reference(tokens, slot_keys, logit_scale, up_weight, up_bias, down_weight, down_bias):
    normed_tok = unit_rms(tokens.astype(jnp.float32), 2).astype(jnp.bfloat16)
    normed_keys = unit_rms(slot_keys.astype(jnp.float32), 0).astype(jnp.bfloat16)
    raw_scores = jnp.einsum('ipd,dn->inp', normed_tok.astype(jnp.float32), normed_keys.astype(jnp.float32))
    logits = logit_scale[0] * raw_scores / D
    dispatch = jax.nn.softmax(logits, axis=2).astype(jnp.bfloat16)
    combine = jax.nn.softmax(logits, axis=1).astype(jnp.bfloat16)
    slot_inputs = jnp.einsum('inp,ipd->ind', dispatch.astype(jnp.float32), tokens.astype(jnp.float32)).astype(jnp.bfloat16)

    def one_expert(packed):
        slot_rows, weight_in, bias_in, weight_out = packed
        pre = jnp.dot(slot_rows, weight_in, preferred_element_type=jnp.float32) + bias_in.astype(jnp.float32)[None, :]
        hidden = jax.nn.gelu(pre, approximate=False).astype(jnp.bfloat16)
        blocks = FF // N_DP
        hidden_blocks = jnp.transpose(hidden.reshape(IMAGES, N_DP, blocks), (1, 0, 2))
        weight_blocks = weight_out.reshape(N_DP, blocks, D)
        parts = jnp.einsum('gif,gfd->gid', hidden_blocks.astype(jnp.float32), weight_blocks.astype(jnp.float32))
        parts = parts.astype(jnp.bfloat16)
        return lax.optimization_barrier(jnp.sum(parts.astype(jnp.float32), axis=0))
    summed = lax.map(one_expert, (jnp.transpose(slot_inputs, (1, 0, 2)), up_weight, up_bias, down_weight))
    expert_out = (summed + down_bias.astype(jnp.float32)[:, None, :]).astype(jnp.bfloat16)
    mixed_out = jnp.einsum('inp,nid->ipd', combine.astype(jnp.float32), expert_out.astype(jnp.float32))
    return mixed_out.astype(jnp.bfloat16)
```

```python
import functools

import jax
import jax.numpy as jnp
from jax import lax
from jax.experimental import pallas as pl
from jax.experimental.pallas import tpu as pltpu
from jax.sharding import PartitionSpec as P

MESH = pl.DeviceIdType.MESH
F32 = jnp.float32
BF16 = jnp.bfloat16
norm_eps = 1e-06
NT = (((1,), (1,)), ((), ()))
CORES = 2


def erf_gelu(v):
    return 0.5 * v * (1.0 + lax.erf(v * 0.7071067811865476))


def route_and_experts(
    owners,
    n_dp,
    chunk,
    tok_hbm,
    keys_ref,
    scale_ref,
    w1_hbm,
    b1_ref,
    w2_hbm,
    b2_ref,
    comb_ref,
    ret_ref,
    tok,
    w1,
    w2,
    send,
    recv,
    xf,
    hid,
    part,
    mine,
    pair,
    back,
    got,
    tok_sem,
    w_sem,
    own_sem,
    s_send,
    s_recv,
    r_send,
    r_recv,
    p_send,
    p_recv,
    b_send,
    b_recv,
):
    images, patches, width = tok.shape
    hidden = w1.shape[1]
    halves = n_dp // CORES
    groups = halves * owners
    rows = groups * images
    slots = owners * images

    d = lax.axis_index("dp")
    e = lax.axis_index("expert")
    core = lax.rem(d, CORES)
    half = lax.div(d, CORES)
    me = half * owners + e
    other = 1 - core
    partner = {"dp": half * CORES + other, "expert": e}

    def device(t):
        return {"dp": lax.div(t, owners) * CORES + core, "expert": lax.rem(t, owners)}

    for i in range(images):
        pltpu.make_async_copy(tok_hbm.at[i], tok.at[i], tok_sem.at[i]).start()
    load1 = pltpu.make_async_copy(w1_hbm.at[0], w1, w_sem.at[0])
    load2 = pltpu.make_async_copy(w2_hbm.at[0], w2, w_sem.at[1])
    load1.start()
    load2.start()

    barrier = pltpu.get_barrier_semaphore()
    pl.semaphore_signal(barrier, inc=1, device_id=partner, device_id_type=MESH)

    def greet(k, c):
        t = lax.rem(me + k, groups)
        pl.semaphore_signal(barrier, inc=1, device_id=device(t), device_id_type=MESH)
        return c

    lax.fori_loop(1, groups, greet, 0)

    keys = keys_ref[...].astype(F32)
    keys = keys * lax.rsqrt(jnp.mean(keys * keys, axis=0, keepdims=True) + norm_eps)
    slot_of = lax.broadcasted_iota(jnp.int32, (slots, owners), 0) // images
    col = lax.broadcasted_iota(jnp.int32, (slots, owners), 1)
    spread = jnp.where(slot_of == col, 1.0, 0.0).astype(BF16)
    keys = lax.dot_general(spread, keys.astype(BF16), NT, preferred_element_type=F32)
    keys = keys.astype(BF16)
    ones = jnp.ones((16, width), BF16)
    factor = scale_ref[0] / width
    image_of = lax.broadcasted_iota(jnp.int32, (slots, patches), 0) % images

    total = None
    for i in range(images):
        pltpu.make_async_copy(tok_hbm.at[i], tok.at[i], tok_sem.at[i]).wait()
        t = tok[i]
        raw = lax.dot_general(keys, t, NT, preferred_element_type=F32)
        squares = lax.dot_general(ones, t * t, NT, preferred_element_type=F32)[0:1]
        logits = raw * (lax.rsqrt(squares / width + norm_eps) * factor)
        keep = image_of == i
        up = jnp.exp(logits - jnp.max(logits, axis=1, keepdims=True))
        up = up / jnp.sum(up, axis=1, keepdims=True)
        dispatch = jnp.where(keep, up, 0.0).astype(BF16)
        term = jnp.dot(dispatch, t, preferred_element_type=F32)
        total = term if total is None else total + term
        mix = jnp.exp(logits - jnp.max(logits, axis=0, keepdims=True))
        mix = mix * (images / jnp.sum(mix, axis=0, keepdims=True))
        comb_ref[i] = jnp.where(keep, mix, 0.0).astype(BF16)
    for n in range(owners):
        send[n] = total[n * images : (n + 1) * images].astype(BF16)

    pl.semaphore_wait(barrier, groups)

    def out_copy(t):
        return pltpu.make_async_remote_copy(
            src_ref=send.at[lax.rem(t, owners)],
            dst_ref=recv.at[core, me],
            send_sem=s_send.at[t],
            recv_sem=s_recv.at[me],
            device_id=device(t),
            device_id_type=MESH,
        )

    def in_copy(t):
        return pltpu.make_async_remote_copy(
            src_ref=send.at[0],
            dst_ref=recv.at[core, t],
            send_sem=s_send.at[t],
            recv_sem=s_recv.at[t],
            device_id=device(t),
            device_id_type=MESH,
        )

    def relay(side, t):
        return pltpu.make_async_remote_copy(
            src_ref=recv.at[side, t],
            dst_ref=recv.at[side, t],
            send_sem=r_send.at[t],
            recv_sem=r_recv.at[t],
            device_id=partner,
            device_id_type=MESH,
        )

    own = pltpu.make_async_copy(send.at[e], recv.at[core, me], own_sem.at[0])
    own.start()

    def start_out(k, c):
        out_copy(lax.rem(me + k, groups)).start()
        return c

    lax.fori_loop(1, groups, start_out, 0)
    own.wait()
    relay(core, me).start()

    def pass_on(k, c):
        t = lax.rem(me + groups - k, groups)
        in_copy(t).wait_recv()
        relay(core, t).start()
        return c

    lax.fori_loop(1, groups, pass_on, 0)

    def take(k, c):
        relay(other, k).wait_recv()
        return c

    lax.fori_loop(0, groups, take, 0)

    for side in range(CORES):

        def place(k, c):
            pairs = [recv[side, 2 * k + q].astype(F32) for q in range(2)]
            at = pl.multiple_of(side * rows + k * 2 * images, 2 * images)
            xf[pl.ds(at, 2 * images), :] = jnp.concatenate(pairs, axis=0)
            return c

        lax.fori_loop(0, groups // 2, place, 0, unroll=groups <= 16)

    load1.wait()
    block = min(128, CORES * rows)
    steps = CORES * rows // block

    def first(m, c):
        at = pl.multiple_of(m * block, block)
        x = xf[pl.ds(at, block), :].astype(BF16)
        for j in range(0, hidden, chunk):
            v = jnp.dot(x, w1[:, j : j + chunk], preferred_element_type=F32)
            v = v + b1_ref[0:1, j : j + chunk].astype(F32)
            hid[pl.ds(at, block), j : j + chunk] = erf_gelu(v).astype(BF16)
        return c

    lax.fori_loop(0, steps, first, 0, unroll=steps == 1)
    load2.wait()

    def pair_copy(j):
        return pltpu.make_async_remote_copy(
            src_ref=part.at[j, other],
            dst_ref=pair.at[j],
            send_sem=p_send.at[j],
            recv_sem=p_recv.at[j],
            device_id=partner,
            device_id_type=MESH,
        )

    pieces = width // chunk
    for j in range(pieces):
        for side in range(CORES):

            def second(m, c):
                at = pl.multiple_of(m * block2, block2)
                h = hid[pl.ds(side * rows + at, block2), :]
                v = jnp.dot(h, w2[:, j * chunk : (j + 1) * chunk], preferred_element_type=F32)
                part[j, side, pl.ds(at, block2), :] = v.astype(BF16)
                mine[j, side, pl.ds(at, block2), :] = v
                return c

            block2 = min(128, rows)
            lax.fori_loop(0, rows // block2, second, 0, unroll=rows == block2)
        pair_copy(j).start()

    for j in range(pieces):
        pair_copy(j).wait_recv()

        def join(k, c):
            at = pl.multiple_of(k * 4 * images, 4 * images)
            v = mine[j, core, pl.ds(at, 4 * images), :]
            v = v + pair[j, pl.ds(at, 4 * images), :].astype(F32)
            for q in range(4):
                back[4 * k + q, :, j * chunk : (j + 1) * chunk] = v[
                    q * images : (q + 1) * images
                ].astype(BF16)
            return c

        lax.fori_loop(0, groups // 4, join, 0, unroll=groups <= 16)

    def home(t):
        return pltpu.make_async_remote_copy(
            src_ref=back.at[t],
            dst_ref=got.at[me],
            send_sem=b_send.at[t],
            recv_sem=b_recv.at[me],
            device_id=device(t),
            device_id_type=MESH,
        )

    def landed(t):
        return pltpu.make_async_remote_copy(
            src_ref=back.at[t],
            dst_ref=got.at[t],
            send_sem=b_send.at[t],
            recv_sem=b_recv.at[t],
            device_id=device(t),
            device_id_type=MESH,
        )

    keep_own = pltpu.make_async_copy(back.at[me], got.at[me], own_sem.at[1])
    keep_own.start()

    def start_home(k, c):
        home(lax.rem(me + k, groups)).start()
        return c

    lax.fori_loop(1, groups, start_home, 0)

    def end_sends(k, c):
        out_copy(lax.rem(me + k, groups)).wait_send()
        return c

    lax.fori_loop(1, groups, end_sends, 0)

    def end_relays(k, c):
        relay(core, k).wait_send()
        return c

    lax.fori_loop(0, groups, end_relays, 0)
    for j in range(pieces):
        pair_copy(j).wait_send()
    keep_own.wait()

    def arrive(k, c):
        landed(lax.rem(me + groups - k, groups)).wait_recv()
        return c

    lax.fori_loop(1, groups, arrive, 0)
    bias = b2_ref[...].astype(F32)
    for n in range(0, owners, 2):
        both = []
        for q in (n, n + 1):
            v = got[q].astype(F32)
            for x in range(1, halves):
                v = v + got[x * owners + q].astype(F32)
            both.append(v + bias[q : q + 1])
        ret_ref[n * images : (n + 2) * images, :] = jnp.concatenate(both, axis=0)

    def end_home(k, c):
        home(lax.rem(me + k, groups)).wait_send()
        return c

    lax.fori_loop(1, groups, end_home, 0)


def mix_kernel(comb_ref, ret_ref, out_ref):
    out_ref[0] = lax.dot_general(
        comb_ref[0],
        ret_ref[...].astype(BF16),
        (((0,), (0,)), ((), ())),
        preferred_element_type=F32,
    ).astype(out_ref.dtype)


def body(tokens, slot_keys, logit_scale, up_weight, up_bias, down_weight, down_bias):
    images, patches, width = tokens.shape
    owners = lax.axis_size("expert")
    n_dp = lax.axis_size("dp")
    hidden = up_weight.shape[2]
    halves = n_dp // CORES
    groups = halves * owners
    rows = groups * images
    slots = owners * images
    chunk = 256
    pieces = width // chunk
    vmem = pl.BlockSpec(memory_space=pltpu.VMEM)
    hbm = pl.BlockSpec(memory_space=pl.ANY)
    dma = pltpu.SemaphoreType.DMA
    comb, ret = pl.pallas_call(
        functools.partial(route_and_experts, owners, n_dp, chunk),
        out_shape=(
            jax.ShapeDtypeStruct((images, slots, patches), BF16),
            jax.ShapeDtypeStruct((slots, width), F32),
        ),
        in_specs=[
            hbm,
            vmem,
            pl.BlockSpec(memory_space=pltpu.SMEM),
            hbm,
            vmem,
            hbm,
            vmem,
        ],
        out_specs=(vmem, vmem),
        scratch_shapes=[
            pltpu.VMEM((images, patches, width), BF16),
            pltpu.VMEM((width, hidden), BF16),
            pltpu.VMEM((hidden, width), BF16),
            pltpu.VMEM((owners, images, width), BF16),
            pltpu.VMEM((CORES, groups, images, width), BF16),
            pltpu.VMEM((CORES * rows, width), F32),
            pltpu.VMEM((CORES * rows, hidden), BF16),
            pltpu.VMEM((pieces, CORES, rows, chunk), BF16),
            pltpu.VMEM((pieces, CORES, rows, chunk), F32),
            pltpu.VMEM((pieces, rows, chunk), BF16),
            pltpu.VMEM((groups, images, width), BF16),
            pltpu.VMEM((groups, images, width), BF16),
            dma((images,)),
            dma((2,)),
            dma((2,)),
            dma((groups,)),
            dma((groups,)),
            dma((groups,)),
            dma((groups,)),
            dma((pieces,)),
            dma((pieces,)),
            dma((groups,)),
            dma((groups,)),
        ],
        compiler_params=pltpu.CompilerParams(
            collective_id=0, has_side_effects=True, vmem_limit_bytes=60 * 1024 * 1024
        ),
        name="route_and_experts",
    )(tokens, slot_keys, logit_scale, up_weight, up_bias, down_weight, down_bias)
    return pl.pallas_call(
        mix_kernel,
        grid=(images,),
        out_shape=jax.ShapeDtypeStruct(tokens.shape, BF16),
        in_specs=[
            pl.BlockSpec((1, slots, patches), lambda i: (i, 0, 0)),
            pl.BlockSpec((slots, width), lambda i: (0, 0)),
        ],
        out_specs=pl.BlockSpec((1, patches, width), lambda i: (i, 0, 0)),
        name="mix_tokens",
    )(comb, ret)


def solution(mesh):
    return jax.shard_map(
        body,
        mesh=mesh,
        in_specs=(
            P(("dp", "expert"), None, None),
            P(),
            P(),
            P("expert", None, "dp"),
            P("expert", "dp"),
            P("expert", "dp", None),
            P(),
        ),
        out_specs=P(("dp", "expert"), None, None),
        check_vma=False,
    )
```

```python
import functools

import jax
import jax.numpy as jnp
from jax import lax
from jax.experimental import pallas as pl
from jax.experimental.pallas import tpu as pltpu
from jax.sharding import PartitionSpec as P

MESH = pl.DeviceIdType.MESH
F32 = jnp.float32
BF16 = jnp.bfloat16
norm_eps = 1e-06
NT = (((1,), (1,)), ((), ()))
CORES = 2


def erf_gelu(v):
    return 0.5 * v * (1.0 + lax.erf(v * 0.7071067811865476))


def route_and_experts(
    owners,
    n_dp,
    chunk,
    tok_hbm,
    keys_hbm,
    scale_hbm,
    w1_hbm,
    b1_hbm,
    w2_hbm,
    b2_hbm,
    comb_ref,
    ret_ref,
    keys_ref,
    scale_ref,
    b1_ref,
    b2_ref,
    tok,
    w1,
    w2,
    send,
    recv,
    xf,
    hid,
    part,
    mine,
    pair,
    back,
    got,
    small_sem,
    tok_sem,
    w_sem,
    own_sem,
    s_send,
    s_recv,
    r_send,
    r_recv,
    p_send,
    p_recv,
    b_send,
    b_recv,
):
    images, patches, width = tok.shape
    hidden = w1.shape[1]
    halves = n_dp // CORES
    groups = halves * owners
    rows = groups * images
    slots = owners * images

    d = lax.axis_index("dp")
    e = lax.axis_index("expert")
    core = lax.rem(d, CORES)
    half = lax.div(d, CORES)
    me = half * owners + e
    other = 1 - core
    partner = {"dp": half * CORES + other, "expert": e}

    quarter = max(1, owners // 4)
    outward = [
        (a, q * quarter + b)
        for q in (2, 3, 1, 0)
        for b in range(quarter)
        for a in reversed(range(halves))
        if q * quarter + b < owners and (a, q * quarter + b) != (0, 0)
    ]
    inward = outward[::-1]

    def for_peers(act, order):
        if groups <= 16:
            for a, b in order:
                act(lax.rem(half + a, halves) * owners + lax.rem(e + b, owners))
        else:

            def step(k, c):
                act(lax.rem(me + k, groups))
                return c

            lax.fori_loop(1, groups, step, 0)

    def device(t):
        return {"dp": lax.div(t, owners) * CORES + core, "expert": lax.rem(t, owners)}

    load_keys = pltpu.make_async_copy(keys_hbm, keys_ref, small_sem.at[0])
    load_scale = pltpu.make_async_copy(scale_hbm, scale_ref, small_sem.at[1])
    load_b1 = pltpu.make_async_copy(b1_hbm, b1_ref, small_sem.at[2])
    load_b2 = pltpu.make_async_copy(b2_hbm, b2_ref, small_sem.at[3])
    load_keys.start()
    load_scale.start()
    for i in range(images):
        pltpu.make_async_copy(tok_hbm.at[i], tok.at[i], tok_sem.at[i]).start()
    load1 = pltpu.make_async_copy(w1_hbm.at[0], w1, w_sem.at[0])
    load2 = pltpu.make_async_copy(w2_hbm.at[0], w2, w_sem.at[1])
    barrier = pltpu.get_barrier_semaphore()
    pl.semaphore_signal(barrier, inc=1, device_id=partner, device_id_type=MESH)

    def greet(k, c):
        t = lax.rem(me + k, groups)
        pl.semaphore_signal(barrier, inc=1, device_id=device(t), device_id_type=MESH)
        return c

    lax.fori_loop(1, groups, greet, 0)

    load_keys.wait()
    keys = keys_ref[...].astype(F32)
    keys = keys * lax.rsqrt(jnp.mean(keys * keys, axis=1, keepdims=True) + norm_eps)
    slot_of = lax.broadcasted_iota(jnp.int32, (slots, owners), 0) // images
    col = lax.broadcasted_iota(jnp.int32, (slots, owners), 1)
    spread = jnp.where(slot_of == col, 1.0, 0.0).astype(BF16)
    keys = jnp.dot(spread, keys.astype(BF16), preferred_element_type=F32)
    keys = keys.astype(BF16)
    ones = jnp.ones((16, width), BF16)
    load_scale.wait()
    factor = scale_ref[0] / width
    image_of = lax.broadcasted_iota(jnp.int32, (slots, patches), 0) % images

    scores = []
    for i in range(images):
        pltpu.make_async_copy(tok_hbm.at[i], tok.at[i], tok_sem.at[i]).wait()
        t = tok[i]
        raw = lax.dot_general(keys, t, NT, preferred_element_type=F32)
        squares = lax.dot_general(ones, t * t, NT, preferred_element_type=F32)[0:1]
        scores.append(raw * (lax.rsqrt(squares / width + norm_eps) * factor))
    load1.start()
    load2.start()
    load_b1.start()
    load_b2.start()
    parts = []
    for i in range(images):
        up = jnp.exp(scores[i] - jnp.max(scores[i], axis=1, keepdims=True))
        up = up / jnp.sum(up, axis=1, keepdims=True)
        parts.append(jnp.where(image_of == i, up, 0.0).astype(BF16))
    total = jnp.zeros((slots, width), F32)
    for i in range(images):
        total = total + jnp.dot(parts[i], tok[i], preferred_element_type=F32)
    for n in range(owners):
        send[n] = total[n * images : (n + 1) * images].astype(BF16)

    pl.semaphore_wait(barrier, groups)

    def out_copy(t):
        return pltpu.make_async_remote_copy(
            src_ref=send.at[lax.rem(t, owners)],
            dst_ref=recv.at[core, me],
            send_sem=s_send.at[t],
            recv_sem=s_recv.at[me],
            device_id=device(t),
            device_id_type=MESH,
        )

    def in_copy(t):
        return pltpu.make_async_remote_copy(
            src_ref=send.at[0],
            dst_ref=recv.at[core, t],
            send_sem=s_send.at[t],
            recv_sem=s_recv.at[t],
            device_id=device(t),
            device_id_type=MESH,
        )

    def relay(side, t):
        return pltpu.make_async_remote_copy(
            src_ref=recv.at[side, t],
            dst_ref=recv.at[side, t],
            send_sem=r_send.at[t],
            recv_sem=r_recv.at[t],
            device_id=partner,
            device_id_type=MESH,
        )

    own = pltpu.make_async_copy(send.at[e], recv.at[core, me], own_sem.at[0])
    own.start()

    def start_out(t):
        out_copy(t).start()

    for_peers(start_out, outward)
    own.wait()
    relay(core, me).start()
    for i in range(images):
        mix = jnp.exp(scores[i] - jnp.max(scores[i], axis=0, keepdims=True))
        mix = mix * (images / jnp.sum(mix, axis=0, keepdims=True))
        comb_ref[i] = jnp.where(image_of == i, mix, 0.0).astype(BF16)

    def pass_on(t):
        in_copy(t).wait_recv()
        relay(core, t).start()

    for_peers(pass_on, inward)

    def take(k, c):
        relay(other, k).wait_recv()
        return c

    lax.fori_loop(0, groups, take, 0)

    for side in range(CORES):

        def place(k, c):
            pairs = [recv[side, 2 * k + q].astype(F32) for q in range(2)]
            at = pl.multiple_of(side * rows + k * 2 * images, 2 * images)
            xf[pl.ds(at, 2 * images), :] = jnp.concatenate(pairs, axis=0)
            return c

        lax.fori_loop(0, groups // 2, place, 0, unroll=groups <= 16)

    load1.wait()
    load_b1.wait()
    load_b2.wait()
    block = min(128, CORES * rows)
    steps = CORES * rows // block

    def first(m, c):
        at = pl.multiple_of(m * block, block)
        x = xf[pl.ds(at, block), :].astype(BF16)
        for j in range(0, hidden, chunk):
            v = jnp.dot(x, w1[:, j : j + chunk], preferred_element_type=F32)
            v = v + b1_ref[0:1, j : j + chunk].astype(F32)
            hid[pl.ds(at, block), j : j + chunk] = erf_gelu(v).astype(BF16)
        return c

    lax.fori_loop(0, steps, first, 0, unroll=steps == 1)
    load2.wait()

    def pair_copy(j):
        return pltpu.make_async_remote_copy(
            src_ref=part.at[j, other],
            dst_ref=pair.at[j],
            send_sem=p_send.at[j],
            recv_sem=p_recv.at[j],
            device_id=partner,
            device_id_type=MESH,
        )

    pieces = width // chunk
    for j in range(pieces):
        for side in range(CORES):

            def second(m, c):
                at = pl.multiple_of(m * block2, block2)
                h = hid[pl.ds(side * rows + at, block2), :]
                v = jnp.dot(h, w2[:, j * chunk : (j + 1) * chunk], preferred_element_type=F32)
                part[j, side, pl.ds(at, block2), :] = v.astype(BF16)
                mine[j, side, pl.ds(at, block2), :] = v
                return c

            block2 = min(128, rows)
            lax.fori_loop(0, rows // block2, second, 0, unroll=rows == block2)
        pair_copy(j).start()

    for j in range(pieces):
        pair_copy(j).wait_recv()

        def join(k, c):
            at = pl.multiple_of(k * 4 * images, 4 * images)
            v = mine[j, core, pl.ds(at, 4 * images), :]
            v = v + pair[j, pl.ds(at, 4 * images), :].astype(F32)
            for q in range(4):
                back[4 * k + q, :, j * chunk : (j + 1) * chunk] = v[
                    q * images : (q + 1) * images
                ].astype(BF16)
            return c

        lax.fori_loop(0, groups // 4, join, 0, unroll=groups <= 16)

    def home(t):
        return pltpu.make_async_remote_copy(
            src_ref=back.at[t],
            dst_ref=got.at[me],
            send_sem=b_send.at[t],
            recv_sem=b_recv.at[me],
            device_id=device(t),
            device_id_type=MESH,
        )

    def landed(t):
        return pltpu.make_async_remote_copy(
            src_ref=back.at[t],
            dst_ref=got.at[t],
            send_sem=b_send.at[t],
            recv_sem=b_recv.at[t],
            device_id=device(t),
            device_id_type=MESH,
        )

    keep_own = pltpu.make_async_copy(back.at[me], got.at[me], own_sem.at[1])
    keep_own.start()

    def start_home(t):
        home(t).start()

    for_peers(start_home, outward)

    def end_sends(k, c):
        out_copy(lax.rem(me + k, groups)).wait_send()
        return c

    lax.fori_loop(1, groups, end_sends, 0)

    def end_relays(k, c):
        relay(core, k).wait_send()
        return c

    lax.fori_loop(0, groups, end_relays, 0)
    for j in range(pieces):
        pair_copy(j).wait_send()
    keep_own.wait()

    def arrive(k, c):
        landed(lax.rem(me + groups - k, groups)).wait_recv()
        return c

    lax.fori_loop(1, groups, arrive, 0)
    bias = b2_ref[...].astype(F32)
    for n in range(0, owners, 2):
        both = []
        for q in (n, n + 1):
            v = got[q].astype(F32)
            for x in range(1, halves):
                v = v + got[x * owners + q].astype(F32)
            both.append(v + bias[q : q + 1])
        ret_ref[n * images : (n + 2) * images, :] = jnp.concatenate(both, axis=0)

    def end_home(k, c):
        home(lax.rem(me + k, groups)).wait_send()
        return c

    lax.fori_loop(1, groups, end_home, 0)


def mix_kernel(comb_ref, ret_ref, out_ref, out, out_sem):
    images = comb_ref.shape[0]
    ret = ret_ref[...].astype(BF16)
    copies = []
    for i in range(images):
        v = lax.dot_general(
            comb_ref[i], ret, (((0,), (0,)), ((), ())), preferred_element_type=F32
        )
        out[i] = v.astype(out.dtype)
        copies.append(pltpu.make_async_copy(out.at[i], out_ref.at[i], out_sem.at[i]))
        copies[-1].start()
    for copy in copies:
        copy.wait()


def body(tokens, slot_keys, logit_scale, up_weight, up_bias, down_weight, down_bias):
    images, patches, width = tokens.shape
    owners = lax.axis_size("expert")
    n_dp = lax.axis_size("dp")
    hidden = up_weight.shape[2]
    halves = n_dp // CORES
    groups = halves * owners
    rows = groups * images
    slots = owners * images
    chunk = 256
    pieces = width // chunk
    vmem = pl.BlockSpec(memory_space=pltpu.VMEM)
    hbm = pl.BlockSpec(memory_space=pl.ANY)
    dma = pltpu.SemaphoreType.DMA
    comb, ret = pl.pallas_call(
        functools.partial(route_and_experts, owners, n_dp, chunk),
        out_shape=(
            pltpu.VMEM((images, slots, patches), BF16),
            pltpu.VMEM((slots, width), F32),
        ),
        in_specs=[
            hbm,
            hbm,
            pl.BlockSpec(memory_space=pltpu.HBM),
            hbm,
            hbm,
            hbm,
            hbm,
        ],
        out_specs=(vmem, vmem),
        scratch_shapes=[
            pltpu.VMEM((owners, width), BF16),
            pltpu.SMEM((1,), F32),
            pltpu.VMEM(up_bias.shape, BF16),
            pltpu.VMEM(down_bias.shape, BF16),
            pltpu.VMEM((images, patches, width), BF16),
            pltpu.VMEM((width, hidden), BF16),
            pltpu.VMEM((hidden, width), BF16),
            pltpu.VMEM((owners, images, width), BF16),
            pltpu.VMEM((CORES, groups, images, width), BF16),
            pltpu.VMEM((CORES * rows, width), F32),
            pltpu.VMEM((CORES * rows, hidden), BF16),
            pltpu.VMEM((pieces, CORES, rows, chunk), BF16),
            pltpu.VMEM((pieces, CORES, rows, chunk), F32),
            pltpu.VMEM((pieces, rows, chunk), BF16),
            pltpu.VMEM((groups, images, width), BF16),
            pltpu.VMEM((groups, images, width), BF16),
            dma((4,)),
            dma((images,)),
            dma((2,)),
            dma((2,)),
            dma((groups,)),
            dma((groups,)),
            dma((groups,)),
            dma((groups,)),
            dma((pieces,)),
            dma((pieces,)),
            dma((groups,)),
            dma((groups,)),
        ],
        compiler_params=pltpu.CompilerParams(
            collective_id=0, has_side_effects=True, vmem_limit_bytes=60 * 1024 * 1024
        ),
        name="route_and_experts",
    )(tokens, slot_keys.T, logit_scale, up_weight, up_bias, down_weight, down_bias)
    return pl.pallas_call(
        mix_kernel,
        out_shape=jax.ShapeDtypeStruct(tokens.shape, BF16),
        in_specs=[vmem, vmem],
        out_specs=hbm,
        scratch_shapes=[pltpu.VMEM(tokens.shape, BF16), dma((images,))],
        name="mix_tokens",
    )(
        pltpu.with_memory_space_constraint(comb, pltpu.VMEM),
        pltpu.with_memory_space_constraint(ret, pltpu.VMEM),
    )


def solution(mesh):
    return jax.shard_map(
        body,
        mesh=mesh,
        in_specs=(
            P(("dp", "expert"), None, None),
            P(),
            P(),
            P("expert", None, "dp"),
            P("expert", "dp"),
            P("expert", "dp", None),
            P(),
        ),
        out_specs=P(("dp", "expert"), None, None),
        check_vma=False,
    )
```

```python
import functools

import jax
import jax.numpy as jnp
from jax import lax
from jax.experimental import pallas as pl
from jax.experimental.pallas import tpu as pltpu
from jax.sharding import PartitionSpec as P

MESH = pl.DeviceIdType.MESH
F32 = jnp.float32
BF16 = jnp.bfloat16
norm_eps = 1e-06
NT = (((1,), (1,)), ((), ()))
CORES = 2


def erf_gelu(v):
    return 0.5 * v * (1.0 + lax.erf(v * 0.7071067811865476))


def route_and_experts(
    owners,
    n_dp,
    chunk,
    tok_hbm,
    keys_hbm,
    scale_hbm,
    w1_hbm,
    b1_hbm,
    w2_hbm,
    b2_hbm,
    comb_ref,
    ret_ref,
    keys_ref,
    scale_ref,
    b1_ref,
    b2_ref,
    tok,
    w1,
    w2,
    send,
    recv,
    xf,
    hid,
    part,
    mine,
    pair,
    back,
    got,
    small_sem,
    tok_sem,
    w_sem,
    own_sem,
    s_send,
    s_recv,
    r_send,
    r_recv,
    p_send,
    p_recv,
    b_send,
    b_recv,
):
    images, patches, width = tok.shape
    hidden = w1.shape[1]
    halves = n_dp // CORES
    groups = halves * owners
    rows = groups * images
    slots = owners * images

    d = lax.axis_index("dp")
    e = lax.axis_index("expert")
    core = lax.rem(d, CORES)
    half = lax.div(d, CORES)
    me = half * owners + e
    other = 1 - core
    partner = {"dp": half * CORES + other, "expert": e}

    quarter = max(1, owners // 4)
    outward = [
        (a, q * quarter + b)
        for q in (2, 3, 1, 0)
        for b in range(quarter)
        for a in reversed(range(halves))
        if q * quarter + b < owners and (a, q * quarter + b) != (0, 0)
    ]
    inward = outward[::-1]

    def for_peers(act, order):
        if groups <= 16:
            for a, b in order:
                act(lax.rem(half + a, halves) * owners + lax.rem(e + b, owners))
        else:

            def step(k, c):
                act(lax.rem(me + k, groups))
                return c

            lax.fori_loop(1, groups, step, 0)

    def device(t):
        return {"dp": lax.div(t, owners) * CORES + core, "expert": lax.rem(t, owners)}

    load_keys = pltpu.make_async_copy(keys_hbm, keys_ref, small_sem.at[0])
    load_scale = pltpu.make_async_copy(scale_hbm, scale_ref, small_sem.at[1])
    load_b1 = pltpu.make_async_copy(b1_hbm, b1_ref, small_sem.at[2])
    load_b2 = pltpu.make_async_copy(b2_hbm, b2_ref, small_sem.at[3])
    load_keys.start()
    load_scale.start()
    for i in range(images):
        pltpu.make_async_copy(tok_hbm.at[i], tok.at[i], tok_sem.at[i]).start()
    load1 = pltpu.make_async_copy(w1_hbm.at[0], w1, w_sem.at[0])
    load2 = pltpu.make_async_copy(w2_hbm.at[0], w2, w_sem.at[1])
    barrier = pltpu.get_barrier_semaphore()
    pl.semaphore_signal(barrier, inc=1, device_id=partner, device_id_type=MESH)

    def greet(k, c):
        t = lax.rem(me + k, groups)
        pl.semaphore_signal(barrier, inc=1, device_id=device(t), device_id_type=MESH)
        return c

    lax.fori_loop(1, groups, greet, 0)

    load_keys.wait()
    keys = keys_ref[...].astype(F32)
    keys = keys * lax.rsqrt(jnp.mean(keys * keys, axis=1, keepdims=True) + norm_eps)
    slot_of = lax.broadcasted_iota(jnp.int32, (slots, owners), 0) // images
    col = lax.broadcasted_iota(jnp.int32, (slots, owners), 1)
    spread = jnp.where(slot_of == col, 1.0, 0.0).astype(BF16)
    keys = jnp.dot(spread, keys.astype(BF16), preferred_element_type=F32)
    keys = keys.astype(BF16)
    ones = jnp.ones((16, width), BF16)
    load_scale.wait()
    factor = scale_ref[0] / width
    image_of = lax.broadcasted_iota(jnp.int32, (slots, patches), 0) % images

    scores = []
    for i in range(images):
        pltpu.make_async_copy(tok_hbm.at[i], tok.at[i], tok_sem.at[i]).wait()
        t = tok[i]
        raw = lax.dot_general(keys, t, NT, preferred_element_type=F32)
        squares = lax.dot_general(ones, t * t, NT, preferred_element_type=F32)[0:1]
        scores.append(raw * (lax.rsqrt(squares / width + norm_eps) * factor))
    load1.start()
    load2.start()
    load_b1.start()
    load_b2.start()
    parts = []
    for i in range(images):
        up = jnp.exp(scores[i] - jnp.max(scores[i], axis=1, keepdims=True))
        up = up / jnp.sum(up, axis=1, keepdims=True)
        parts.append(jnp.where(image_of == i, up, 0.0).astype(BF16))
    total = jnp.zeros((slots, width), F32)
    for i in range(images):
        total = total + jnp.dot(parts[i], tok[i], preferred_element_type=F32)
    for n in range(owners):
        send[n] = total[n * images : (n + 1) * images].astype(BF16)

    pl.semaphore_wait(barrier, groups)

    def out_copy(t):
        return pltpu.make_async_remote_copy(
            src_ref=send.at[lax.rem(t, owners)],
            dst_ref=recv.at[core, me],
            send_sem=s_send.at[t],
            recv_sem=s_recv.at[me],
            device_id=device(t),
            device_id_type=MESH,
        )

    def in_copy(t):
        return pltpu.make_async_remote_copy(
            src_ref=send.at[0],
            dst_ref=recv.at[core, t],
            send_sem=s_send.at[t],
            recv_sem=s_recv.at[t],
            device_id=device(t),
            device_id_type=MESH,
        )

    def relay(side, t):
        return pltpu.make_async_remote_copy(
            src_ref=recv.at[side, t],
            dst_ref=recv.at[side, t],
            send_sem=r_send.at[t],
            recv_sem=r_recv.at[t],
            device_id=partner,
            device_id_type=MESH,
        )

    own = pltpu.make_async_copy(send.at[e], recv.at[core, me], own_sem.at[0])
    own.start()

    def start_out(t):
        out_copy(t).start()

    for_peers(start_out, outward)
    own.wait()
    relay(core, me).start()
    for i in range(images):
        mix = jnp.exp(scores[i] - jnp.max(scores[i], axis=0, keepdims=True))
        mix = mix * (images / jnp.sum(mix, axis=0, keepdims=True))
        comb_ref[i] = jnp.where(image_of == i, mix, 0.0).astype(BF16)

    def pass_on(t):
        in_copy(t).wait_recv()
        relay(core, t).start()

    for_peers(pass_on, inward)

    def take(k, c):
        relay(other, k).wait_recv()
        return c

    lax.fori_loop(0, groups, take, 0)

    for side in range(CORES):

        def place(k, c):
            pairs = [recv[side, 2 * k + q].astype(F32) for q in range(2)]
            at = pl.multiple_of(side * rows + k * 2 * images, 2 * images)
            xf[pl.ds(at, 2 * images), :] = jnp.concatenate(pairs, axis=0)
            return c

        lax.fori_loop(0, groups // 2, place, 0, unroll=groups <= 16)

    load1.wait()
    load_b1.wait()
    load_b2.wait()
    block = min(128, CORES * rows)
    steps = CORES * rows // block

    def first(m, c):
        at = pl.multiple_of(m * block, block)
        x = xf[pl.ds(at, block), :].astype(BF16)
        for j in range(0, hidden, chunk):
            v = jnp.dot(x, w1[:, j : j + chunk], preferred_element_type=F32)
            v = v + b1_ref[0:1, j : j + chunk].astype(F32)
            hid[pl.ds(at, block), j : j + chunk] = erf_gelu(v).astype(BF16)
        return c

    lax.fori_loop(0, steps, first, 0, unroll=steps == 1)
    load2.wait()

    def pair_copy(j):
        return pltpu.make_async_remote_copy(
            src_ref=part.at[j, pl.ds(pl.multiple_of(other * rows, rows), rows)],
            dst_ref=pair.at[j],
            send_sem=p_send.at[j],
            recv_sem=p_recv.at[j],
            device_id=partner,
            device_id_type=MESH,
        )

    pieces = width // chunk
    for j in range(pieces):

        def second(m, c):
            at = pl.multiple_of(m * block, block)
            h = hid[pl.ds(at, block), :]
            v = jnp.dot(h, w2[:, j * chunk : (j + 1) * chunk], preferred_element_type=F32)
            part[j, pl.ds(at, block), :] = v.astype(BF16)
            mine[j, pl.ds(at, block), :] = v
            return c

        lax.fori_loop(0, steps, second, 0, unroll=steps == 1)
        pair_copy(j).start()

    for j in range(pieces):
        pair_copy(j).wait_recv()

        def join(k, c):
            at = pl.multiple_of(k * 4 * images, 4 * images)
            own_at = pl.multiple_of(core * rows + at, 4 * images)
            v = mine[j, pl.ds(own_at, 4 * images), :]
            v = v + pair[j, pl.ds(at, 4 * images), :].astype(F32)
            for q in range(4):
                back[4 * k + q, :, j * chunk : (j + 1) * chunk] = v[
                    q * images : (q + 1) * images
                ].astype(BF16)
            return c

        lax.fori_loop(0, groups // 4, join, 0, unroll=groups <= 16)

    def home(t):
        return pltpu.make_async_remote_copy(
            src_ref=back.at[t],
            dst_ref=got.at[me],
            send_sem=b_send.at[t],
            recv_sem=b_recv.at[me],
            device_id=device(t),
            device_id_type=MESH,
        )

    def landed(t):
        return pltpu.make_async_remote_copy(
            src_ref=back.at[t],
            dst_ref=got.at[t],
            send_sem=b_send.at[t],
            recv_sem=b_recv.at[t],
            device_id=device(t),
            device_id_type=MESH,
        )

    keep_own = pltpu.make_async_copy(back.at[me], got.at[me], own_sem.at[1])
    keep_own.start()

    def start_home(t):
        home(t).start()

    for_peers(start_home, outward)

    def end_sends(k, c):
        out_copy(lax.rem(me + k, groups)).wait_send()
        return c

    lax.fori_loop(1, groups, end_sends, 0)

    def end_relays(k, c):
        relay(core, k).wait_send()
        return c

    lax.fori_loop(0, groups, end_relays, 0)
    for j in range(pieces):
        pair_copy(j).wait_send()
    keep_own.wait()

    def arrive(k, c):
        landed(lax.rem(me + groups - k, groups)).wait_recv()
        return c

    lax.fori_loop(1, groups, arrive, 0)
    bias = b2_ref[...].astype(F32)
    for n in range(0, owners, 2):
        both = []
        for q in (n, n + 1):
            v = got[q].astype(F32)
            for x in range(1, halves):
                v = v + got[x * owners + q].astype(F32)
            both.append(v + bias[q : q + 1])
        ret_ref[n * images : (n + 2) * images, :] = jnp.concatenate(both, axis=0)

    def end_home(k, c):
        home(lax.rem(me + k, groups)).wait_send()
        return c

    lax.fori_loop(1, groups, end_home, 0)


def mix_kernel(comb_ref, ret_ref, out_ref, out, out_sem):
    images = comb_ref.shape[0]
    ret = ret_ref[...].astype(BF16)
    copies = []
    for i in range(images):
        v = lax.dot_general(
            comb_ref[i], ret, (((0,), (0,)), ((), ())), preferred_element_type=F32
        )
        out[i] = v.astype(out.dtype)
        copies.append(pltpu.make_async_copy(out.at[i], out_ref.at[i], out_sem.at[i]))
        copies[-1].start()
    for copy in copies:
        copy.wait()


def body(tokens, slot_keys, logit_scale, up_weight, up_bias, down_weight, down_bias):
    images, patches, width = tokens.shape
    owners = lax.axis_size("expert")
    n_dp = lax.axis_size("dp")
    hidden = up_weight.shape[2]
    halves = n_dp // CORES
    groups = halves * owners
    rows = groups * images
    slots = owners * images
    chunk = 256
    pieces = width // chunk
    vmem = pl.BlockSpec(memory_space=pltpu.VMEM)
    hbm = pl.BlockSpec(memory_space=pl.ANY)
    dma = pltpu.SemaphoreType.DMA
    comb, ret = pl.pallas_call(
        functools.partial(route_and_experts, owners, n_dp, chunk),
        out_shape=(
            pltpu.VMEM((images, slots, patches), BF16),
            pltpu.VMEM((slots, width), F32),
        ),
        in_specs=[
            hbm,
            hbm,
            pl.BlockSpec(memory_space=pltpu.HBM),
            hbm,
            hbm,
            hbm,
            hbm,
        ],
        out_specs=(vmem, vmem),
        scratch_shapes=[
            pltpu.VMEM((owners, width), BF16),
            pltpu.SMEM((1,), F32),
            pltpu.VMEM(up_bias.shape, BF16),
            pltpu.VMEM(down_bias.shape, BF16),
            pltpu.VMEM((images, patches, width), BF16),
            pltpu.VMEM((width, hidden), BF16),
            pltpu.VMEM((hidden, width), BF16),
            pltpu.VMEM((owners, images, width), BF16),
            pltpu.VMEM((CORES, groups, images, width), BF16),
            pltpu.VMEM((CORES * rows, width), F32),
            pltpu.VMEM((CORES * rows, hidden), BF16),
            pltpu.VMEM((pieces, CORES * rows, chunk), BF16),
            pltpu.VMEM((pieces, CORES * rows, chunk), F32),
            pltpu.VMEM((pieces, rows, chunk), BF16),
            pltpu.VMEM((groups, images, width), BF16),
            pltpu.VMEM((groups, images, width), BF16),
            dma((4,)),
            dma((images,)),
            dma((2,)),
            dma((2,)),
            dma((groups,)),
            dma((groups,)),
            dma((groups,)),
            dma((groups,)),
            dma((pieces,)),
            dma((pieces,)),
            dma((groups,)),
            dma((groups,)),
        ],
        compiler_params=pltpu.CompilerParams(
            collective_id=0, has_side_effects=True, vmem_limit_bytes=60 * 1024 * 1024
        ),
        name="route_and_experts",
    )(tokens, slot_keys.T, logit_scale, up_weight, up_bias, down_weight, down_bias)
    return pl.pallas_call(
        mix_kernel,
        out_shape=jax.ShapeDtypeStruct(tokens.shape, BF16),
        in_specs=[vmem, vmem],
        out_specs=hbm,
        scratch_shapes=[pltpu.VMEM(tokens.shape, BF16), dma((images,))],
        name="mix_tokens",
    )(
        pltpu.with_memory_space_constraint(comb, pltpu.VMEM),
        pltpu.with_memory_space_constraint(ret, pltpu.VMEM),
    )


def solution(mesh):
    return jax.shard_map(
        body,
        mesh=mesh,
        in_specs=(
            P(("dp", "expert"), None, None),
            P(),
            P(),
            P("expert", None, "dp"),
            P("expert", "dp"),
            P("expert", "dp", None),
            P(),
        ),
        out_specs=P(("dp", "expert"), None, None),
        check_vma=False,
    )
```
